32 devices in a mesh: row: 8 (over z, x), col: 4 (over y, core).
Axes of the slice: x: 2, y: 2, z: 4, core: 2. Of those that a mesh axis runs over, the one named last changes fastest.
Arguments:
- factor: float32 [9, 1024, 3, 512], P(None, 'row', None, 'col'), may hold values from -2 to 2.5, as said below
- adjoint: float32 [9, 1024, 3, 512], P(None, 'row', None, 'col'), may hold values from -6 to 6
Outputs:
- kernel_adjoint: float32 [9, 1024, 3, 512], P(None, 'row', None, 'col')
The draws below stay inside these ranges and needn't reach their ends.
Inputs may be any that keep to these rules, and one draw needn't show every extreme that they name: `factor`: zero where the column minus 512 exceeds the row; the diagonal entries of the two 512-square diagonal blocks lie between 1 and 2.5.
All inputs are finite; a program needn't handle non-finite values.
Results may differ from the reference program's by a relative error of at most 0.0001.
Values sent between devices are 32-bit elements; how exact they have to be, the bound alone decides.
A program may use at most 64 MiB of HBM per device.

```python
import jax
import jax.numpy as jnp
from jax import lax

NB = 512
RC = 9
CC = 3
RW = 1024
CW = 512
NR = 9216
NC = 1536
LEFT = 512


def draw_factor(key, part):
    key_base = jax.random.fold_in(key, 11)
    key_diag = jax.random.fold_in(key, 12)
    raw_draw = jnp.clip(jax.random.normal(key_base, (NR, NC), jnp.float32), -6.0, 6.0)
    diag_values = jax.random.uniform(key_diag, (NR, 1), jnp.float32, 1.0, 2.0)
    row_ids = jnp.arange(NR, dtype=jnp.int32)[:, None]
    col_ids = jnp.arange(NC, dtype=jnp.int32)[None, :] - LEFT
    panel_rows = row_ids < 2 * NB
    scale_map = jnp.where(panel_rows, NB ** (-0.5), NR ** (-0.5))
    same_block = (col_ids >= 0) & (col_ids // NB == row_ids // NB) & panel_rows
    scale_map = jnp.where(same_block, 0.4 * NB ** (-0.5), scale_map)
    values = raw_draw * scale_map
    values = jnp.where(same_block & (col_ids == row_ids), diag_values, values)
    values = jnp.where(col_ids > row_ids, 0.0, values)
    return values.reshape(RC, RW, CC, CW)


def steps_of(key, dims, pieces, least, high):
    factor_of, own = 1.0, jax.random.fold_in(key, 6)
    for dim, blocks in pieces:
        steps = jnp.exp(jax.random.uniform(jax.random.fold_in(own, dim), (blocks,), jnp.float32, least / len(pieces), high / len(pieces)))
        factor_of = factor_of * jnp.repeat(steps, dims[dim] // blocks).reshape([-1 if axis == dim else 1 for axis in range(len(dims))])
    return factor_of


def bell_draw(rng, shape, scale, limit, pieces=(), held_as=jnp.bfloat16):
    result = scale * jax.random.normal(rng, shape, jnp.float32)
    if pieces:
        result = result * steps_of(rng, shape, pieces, -0.22, 0.18)
    return jnp.clip(result, -limit, limit).astype(held_as)


def setup_inputs(seed: int = 0) -> dict:
    streams_of = jax.random.split(jax.random.key(seed), 3)
    return {
        "factor": draw_factor(jax.random.fold_in(streams_of[2], 71), 0),
        "adjoint": bell_draw(streams_of[1], (RC, RW, CC, CW), 1.0, 6.0, ((1, 8), (3, 4)), jnp.float32),
    }


def exact_dot(first, second):
    return jnp.dot(first.astype(jnp.float32), second.astype(jnp.float32), precision=lax.Precision.HIGHEST, preferred_element_type=jnp.float32)

def lower_half(matrix):
    return jnp.tril(matrix) - 0.5 * jnp.diag(jnp.diag(matrix))

def reference(factor, adjoint):
    factor_mat = factor.reshape(NR, NC)
    row_ids = jnp.arange(NR, dtype=jnp.int32)[:, None]
    col_ids = jnp.arange(NC, dtype=jnp.int32)[None, :]
    working = jnp.where(col_ids - LEFT > row_ids, 0.0, adjoint.reshape(NR, NC))
    for panel_index in (1,):
        first_row = panel_index * NB
        bottom = first_row + NB
        first_col = LEFT + first_row
        last_col = first_col + NB
        diag_block = factor_mat[first_row:bottom, first_col:last_col]
        row_block = factor_mat[first_row:bottom, :first_col]
        trail_block = factor_mat[bottom:, :first_col]
        panel_block = factor_mat[bottom:, first_col:last_col]
        column_adjoint = lax.linalg.triangular_solve(diag_block, working[bottom:, first_col:last_col], left_side=False, lower=True)
        trail_adjoint = working[bottom:, :first_col] - exact_dot(column_adjoint, row_block)
        diag_start = working[first_row:bottom, first_col:last_col] - jnp.tril(exact_dot(column_adjoint.T, panel_block))
        product = lower_half(exact_dot(diag_block.T, diag_start))
        left_solved = lax.linalg.triangular_solve(diag_block, product, left_side=True, lower=True, transpose_a=True)
        symmetric = lax.linalg.triangular_solve(diag_block, left_solved, left_side=False, lower=True)
        diag_adjoint = lower_half(symmetric + symmetric.T)
        row_adjoint = working[first_row:bottom, :first_col] - exact_dot(column_adjoint.T, trail_block) - exact_dot(diag_adjoint + diag_adjoint.T, row_block)
        working = working.at[bottom:, first_col:last_col].set(column_adjoint)
        working = working.at[bottom:, :first_col].set(trail_adjoint)
        working = working.at[first_row:bottom, first_col:last_col].set(diag_adjoint)
        working = working.at[first_row:bottom, :first_col].set(row_adjoint)
    return working.reshape(RC, RW, CC, CW)
```

```python
import functools

import jax
import jax.numpy as jnp
from jax import lax
from jax.experimental import pallas as pl
from jax.experimental.pallas import tpu as pltpu
from jax.sharding import PartitionSpec as P

NB = 512
LANES = 128
MESH = pl.DeviceIdType.MESH


def dot(first, second, first_dim=1):
    return lax.dot_general(
        first,
        second,
        (((first_dim,), (0,)), ((), ())),
        precision=lax.Precision.HIGHEST,
        preferred_element_type=jnp.float32,
    )


def iota(shape, dim):
    return lax.broadcasted_iota(jnp.int32, shape, dim)


class Plan:
    def __init__(self, rows, cols, shape):
        self.rows, self.cols = rows, cols
        self.cycles, self.col_cycles, self.tile, _ = shape
        self.nx = 1
        while 2 * (2 * self.nx) ** 2 <= rows:
            self.nx *= 2
        self.nz = rows // self.nx
        self.owners = NB // self.tile
        self.owner_z = self.owners // self.nx
        self.panels = NB // LANES
        self.ny = cols // 2
        self.left = self.col_cycles * cols * LANES - 2 * NB


class ColumnGather:
    def __init__(self, plan, col, full, send, pair, forward, recv):
        self.plan, self.col, self.full = plan, col, full
        self.send, self.pair, self.forward, self.recv = send, pair, forward, recv
        self.first = plan.cols - plan.panels
        self.y, self.core = col // 2, col % 2
        self.mine = col - self.first

    def slot(self, block):
        return self.full.at[:, :, pl.ds(pl.multiple_of(block * LANES, LANES), LANES)]

    def copy(self, src, block, send, col):
        return pltpu.make_async_remote_copy(
            src_ref=src,
            dst_ref=self.slot(block),
            send_sem=send,
            recv_sem=self.recv.at[block],
            device_id={"col": col},
            device_id_type=MESH,
        )

    def other(self, step):
        return (self.y + step) % self.plan.ny

    def copies(self, src):
        out = [
            self.copy(src, self.mine, self.send.at[step], self.other(step) * 2 + self.core)
            for step in range(1, self.plan.ny)
        ]
        out.append(self.copy(src, self.mine, self.pair, self.y * 2 + 1 - self.core))
        return out

    def own(self, src):
        return pltpu.make_async_copy(src, self.slot(self.mine), self.recv.at[self.mine])

    def start(self, src):
        @pl.when(self.mine >= 0)
        def _():
            for copy in self.copies(src):
                copy.start()
            self.own(src).start()

    def relay(self):
        for step in range(1, self.plan.ny):
            block = self.other(step) * 2 + self.core - self.first

            @pl.when(block >= 0)
            def _():
                copy = self.copy(
                    self.slot(block), block, self.forward.at[step], self.y * 2 + 1 - self.core
                )
                copy.wait_recv()
                copy.start()

    def finish(self, src):
        @pl.when(self.mine >= 0)
        def _():
            self.own(src).wait()

        for step in range(self.plan.ny):
            block = self.other(step) * 2 + 1 - self.core - self.first

            @pl.when(block >= 0)
            def _():
                self.copy(self.slot(block), block, self.pair, self.y * 2 + 1 - self.core).wait_recv()

    def drain(self, src):
        @pl.when(self.mine >= 0)
        def _():
            for copy in self.copies(src):
                copy.wait_send()

        for step in range(1, self.plan.ny):
            block = self.other(step) * 2 + self.core - self.first

            @pl.when(block >= 0)
            def _():
                self.copy(
                    self.slot(block), block, self.forward.at[step], self.y * 2 + 1 - self.core
                ).wait_send()


def invert(full, inverse):
    row, col = iota((LANES, LANES), 0), iota((LANES, LANES), 1)
    count = NB // LANES
    blocks = []
    for k in range(count):
        part = full[k * LANES : (k + 1) * LANES, k * LANES : (k + 1) * LANES]
        blocks.append((part, jnp.where(row == col, 1.0 / jnp.where(row == col, part, 1.0), 0.0)))
    size = 1
    while size < LANES:
        mask = (
            (row // (2 * size) == col // (2 * size))
            & (row // size % 2 == 1)
            & (col // size % 2 == 0)
        )
        half = [dot(jnp.where(mask, part, 0.0), inv) for part, inv in blocks]
        blocks = [(part, inv - dot(inv, other)) for (part, inv), other in zip(blocks, half)]
        size *= 2
    inverse[...] = jnp.zeros_like(inverse)
    for k in range(count):
        inverse[k * LANES : (k + 1) * LANES, k * LANES : (k + 1) * LANES] = blocks[k][1]
    while size < NB:
        for base in range(0, NB, 2 * size):
            top, low = slice(base, base + size), slice(base + size, base + 2 * size)
            inner = dot(full[low, top], inverse[top, top])
            inverse[low, top] = -dot(inverse[low, low], inner)
        size *= 2


def kernel(
    plan, factor, adjoint, out,
    panel, top, diag, inv, inv_t, corner, spread, yval, ysum, xrecv, zrecv, starts, start_full,
    a_send, a_pair, a_fwd, a_recv, d_send, d_pair, d_fwd, d_recv,
    s_send, s_pair, s_fwd, s_recv,
    t_z, t_x, t_fwd, t_recv, x_send, x_recv, z_send, z_recv, r_send, r_recv,
):
    p = plan
    row, col = lax.axis_index("row"), lax.axis_index("col")
    z, x = row // p.nx, row % p.nx
    last = p.col_cycles - 1
    tile, depth = p.tile, (p.cycles - 1) * p.tile
    width = p.col_cycles * LANES
    owner = row - (p.rows - p.owners)
    first_z = p.nz - p.owner_z
    is_panel = col >= p.cols - p.panels
    mine = col - (p.cols - p.panels)
    order = [last] + list(range(last))

    barrier = pltpu.get_barrier_semaphore()
    for step in range(1, p.rows):
        pl.semaphore_signal(
            barrier, inc=1, device_id={"row": (row + step) % p.rows}, device_id_type=MESH
        )
    for step in range(1, p.cols):
        pl.semaphore_signal(
            barrier, inc=1, device_id={"col": (col + step) % p.cols}, device_id_type=MESH
        )
    pl.semaphore_wait(barrier, p.rows + p.cols - 2)

    def to_row(src, dst, send, recv, target):
        return pltpu.make_async_remote_copy(
            src_ref=src, dst_ref=dst, send_sem=send, recv_sem=recv,
            device_id={"row": target}, device_id_type=MESH,
        )

    gather_a = ColumnGather(p, col, panel, a_send, a_pair, a_fwd, a_recv)
    a_src = adjoint.at[1:, last]
    gather_a.start(a_src)

    def top_slot(index, e):
        return top.at[index, :, e * LANES : (e + 1) * LANES]

    def top_copies(e):
        src = factor.at[0, e]
        dst, recv = top_slot(owner, e), t_recv.at[e, owner]
        made = [
            to_row(src, dst, t_z.at[e, k], recv, (z + k) % p.nz * p.nx + x) for k in range(1, p.nz)
        ]
        return made + [
            to_row(src, dst, t_x.at[e, k], recv, z * p.nx + (x + k) % p.nx) for k in range(1, p.nx)
        ]

    def top_own(e):
        return pltpu.make_async_copy(factor.at[0, e], top_slot(owner, e), t_recv.at[e, owner])

    @pl.when(owner >= 0)
    def _():
        for e in order:
            for copy in top_copies(e):
                copy.start()
            top_own(e).start()

    def top_forward(e, zi, action):
        index = zi * p.nx + x

        @pl.when(z != first_z + zi)
        def _():
            slot = top_slot(index, e)
            for k in range(1, p.nx):
                copy = to_row(
                    slot, slot, t_fwd.at[e, zi, k], t_recv.at[e, index],
                    z * p.nx + (x + k) % p.nx,
                )
                action(copy, k)

    def relay(copy, k):
        if k == 1:
            copy.wait_recv()
        copy.start()

    def top_relay(e):
        for zi in range(p.owner_z):
            top_forward(e, zi, relay)

    def top_finish(e):
        @pl.when(owner >= 0)
        def _():
            top_own(e).wait()

        for zi in range(p.owner_z):
            for k in range(1, p.nx):
                index = zi * p.nx + (x + k) % p.nx
                slot = top_slot(index, e)
                to_row(slot, slot, t_x.at[e, k], t_recv.at[e, index], row).wait_recv()

    top_relay(last)
    top_finish(last)
    gather_d = ColumnGather(p, col, diag, d_send, d_pair, d_fwd, d_recv)
    d_src = top.at[:, :, last * LANES : width]
    gather_d.start(d_src)
    gather_a.relay()
    for e in range(last):
        top_relay(e)
    gather_d.relay()
    gather_a.finish(a_src)

    a_full = panel[...].reshape(depth, NB)
    columns = [factor[1:, e].reshape(depth, LANES) for e in range(p.col_cycles)]
    corner[...] = dot(a_full, jnp.concatenate(columns, 1), 0)

    gather_d.finish(d_src)
    full = diag.reshape(NB, NB)
    invert(full, inv)
    inv_t[...] = inv[...].T.reshape(inv_t.shape)

    def x_copy(e, k):
        target = (x + k) % p.nx
        return to_row(
            yval.at[e, target], xrecv.at[e, x], x_send.at[e, k], x_recv.at[e, x],
            z * p.nx + target,
        )

    inv_tv = inv_t[...].reshape(NB, NB)

    def put(e, value):
        value = value.reshape(p.owner_z, p.nx, tile, LANES)
        for k in range(p.nx):
            yval[e, k] = value[:, k]
        for k in range(1, p.nx):
            x_copy(e, k).start()

    put(last, dot(inv_tv, corner[:, last * LANES : width]))
    rest = dot(inv_tv, corner[:, : last * LANES])
    for e in range(last):
        put(e, rest[:, e * LANES : (e + 1) * LANES])

    def z_copy(e, zi):
        return to_row(
            ysum.at[e, zi], zrecv.at[e, z], z_send.at[e, zi], z_recv.at[e, z],
            (first_z + zi) * p.nx + x,
        )

    def x_sum(e):
        total = yval[e, x]
        for k in range(1, p.nx):
            source = (x + k) % p.nx
            to_row(
                xrecv.at[e, source], xrecv.at[e, source], x_send.at[e, k], x_recv.at[e, source], row
            ).wait_recv()
            total = total + xrecv[e, source]
        ysum[e] = total
        for zi in range(p.owner_z):
            @pl.when(z != first_z + zi)
            def _():
                z_copy(e, zi).start()

    x_sum(last)
    for e in range(last):
        top_finish(e)
    rights = top[...].reshape(NB, width)
    unit = (iota((NB, LANES), 0) == mine * LANES + iota((NB, LANES), 1)).astype(jnp.float32)
    rights = jnp.concatenate(
        [rights[:, : last * LANES], jnp.where(is_panel, unit, rights[:, last * LANES :])], 1
    )
    spread[...] = dot(inv[...], rights)
    for e in range(last):
        x_sum(e)

    def trail(begin, end):
        change = dot(panel[begin:end].reshape((end - begin) * tile, NB), spread[...])
        change = change.reshape(end - begin, tile, width)
        for e in range(p.col_cycles):
            part = change[:, :, e * LANES : (e + 1) * LANES]
            moved = adjoint[1 + begin : 1 + end, e] - part
            if e == last:
                moved = jnp.where(is_panel, part, moved)
            out[1 + begin : 1 + end, e] = moved

    middle = (p.cycles - 1) // 2
    trail(0, middle)

    def z_sum(e):
        total = ysum[e, owner // p.nx]
        for k in range(1, p.nz):
            source = (z + k) % p.nz
            to_row(
                zrecv.at[e, source], zrecv.at[e, source], z_send.at[e, 0], z_recv.at[e, source], row
            ).wait_recv()
            total = total + zrecv[e, source]
        return total

    def start_copies():
        first = p.rows - p.owners
        return [
            to_row(
                starts.at[owner], starts.at[owner], r_send.at[k], r_recv.at[owner],
                first + (owner + k) % p.owners,
            )
            for k in range(1, p.owners)
        ]

    lower = iota((tile, LANES), 0) + owner * tile >= iota((tile, LANES), 1) + mine * LANES
    gather_s = ColumnGather(p, col, start_full, s_send, s_pair, s_fwd, s_recv)

    @pl.when((owner >= 0) & is_panel)
    def _():
        starts[owner] = jnp.where(lower, adjoint[0, last] - z_sum(last), 0.0)
        for copy in start_copies():
            copy.start()

    trail(middle, p.cycles - 1)

    @pl.when(owner < 0)
    def _():
        for e in range(p.col_cycles):
            rows_at = iota((tile, LANES), 0) + row * tile
            cols_at = iota((tile, LANES), 1) + (e * p.cols + col) * LANES - p.left
            out[0, e] = jnp.where(cols_at > rows_at, 0.0, adjoint[0, e])

    @pl.when(owner >= 0)
    def _():
        @pl.when(is_panel)
        def _():
            for k in range(1, p.owners):
                source = (owner + k) % p.owners
                to_row(
                    starts.at[source], starts.at[source], r_send.at[k], r_recv.at[source], row
                ).wait_recv()

        gather_s.start(starts)
        gather_s.relay()
        gather_s.finish(starts)
        product = dot(full[...], start_full[...].reshape(NB, NB), 0)
        row_at, col_at = iota((NB, NB), 0), iota((NB, NB), 1)
        both = (
            jnp.where(row_at >= col_at, product, 0.0) + jnp.where(row_at > col_at, product, 0.0).T
        )
        changes = dot(dot(inv_t[owner], both), spread[...])
        for e in range(last):
            out[0, e] = adjoint[0, e] - z_sum(e) - changes[:, e * LANES : (e + 1) * LANES]

        part = changes[:, last * LANES :]

        @pl.when(is_panel)
        def _():
            equal = iota((tile, LANES), 0) + owner * tile == iota((tile, LANES), 1) + mine * LANES
            out[0, last] = jnp.where(lower, jnp.where(equal, 0.5 * part, part), 0.0)

        @pl.when(jnp.logical_not(is_panel))
        def _():
            out[0, last] = adjoint[0, last] - z_sum(last) - part

        gather_s.drain(starts)

        @pl.when(is_panel)
        def _():
            for copy in start_copies():
                copy.wait_send()

    gather_a.drain(a_src)
    gather_d.drain(d_src)
    for e in order:
        @pl.when(owner >= 0)
        def _():
            for copy in top_copies(e):
                copy.wait_send()

        for zi in range(p.owner_z):
            top_forward(e, zi, lambda copy, k: copy.wait_send())

            @pl.when(z != first_z + zi)
            def _():
                z_copy(e, zi).wait_send()

        for k in range(1, p.nx):
            x_copy(e, k).wait_send()


def local(rows, cols, factor, adjoint):
    factor = jnp.transpose(factor, (0, 2, 1, 3))
    adjoint = jnp.transpose(adjoint, (0, 2, 1, 3))
    p = Plan(rows, cols, factor.shape)
    n, cc, tile = p.cycles - 1, p.col_cycles, p.tile
    dma = pltpu.SemaphoreType.DMA
    column = [dma((p.ny,)), dma, dma((p.ny,)), dma((p.panels,))]
    vmem = lambda *shape: pltpu.VMEM(shape, jnp.float32)
    result = pl.pallas_call(
        functools.partial(kernel, p),
        out_shape=jax.ShapeDtypeStruct(factor.shape, jnp.float32),
        in_specs=[pl.BlockSpec(memory_space=pltpu.VMEM)] * 2,
        out_specs=pl.BlockSpec(memory_space=pltpu.VMEM),
        scratch_shapes=[
            vmem(n, tile, NB),
            vmem(p.owners, tile, cc * LANES),
            vmem(p.owners, tile, NB),
            vmem(NB, NB),
            vmem(p.owners, tile, NB),
            vmem(NB, cc * LANES),
            vmem(NB, cc * LANES),
            vmem(cc, p.nx, p.owner_z, tile, LANES),
            vmem(cc, p.owner_z, tile, LANES),
            vmem(cc, p.nx, p.owner_z, tile, LANES),
            vmem(cc, p.nz, tile, LANES),
            vmem(p.owners, tile, LANES),
            vmem(p.owners, tile, NB),
            *column, *column, *column,
            dma((cc, p.nz)), dma((cc, p.nx)), dma((cc, p.owner_z, p.nx)), dma((cc, p.owners)),
            dma((cc, p.nx)), dma((cc, p.nx)), dma((cc, p.owner_z)), dma((cc, p.nz)),
            dma((p.owners,)), dma((p.owners,)),
        ],
        compiler_params=pltpu.CompilerParams(
            collective_id=0, has_side_effects=True, vmem_limit_bytes=48 * 1024 * 1024
        ),
    )(factor, adjoint)
    return jnp.transpose(result, (0, 2, 1, 3))


def solution(mesh):
    spec = P(None, "row", None, "col")
    step = functools.partial(local, mesh.shape["row"], mesh.shape["col"])
    return jax.shard_map(
        step, mesh=mesh, in_specs=(spec, spec), out_specs=spec, check_vma=False
    )
```

```python
import functools

import jax
import jax.numpy as jnp
from jax import lax
from jax.experimental import pallas as pl
from jax.experimental.pallas import tpu as pltpu
from jax.sharding import PartitionSpec as P

NB = 512
LANES = 128
MESH = pl.DeviceIdType.MESH


def dot(first, second, first_dim=1):
    return lax.dot_general(
        first,
        second,
        (((first_dim,), (0,)), ((), ())),
        precision=lax.Precision.HIGHEST,
        preferred_element_type=jnp.float32,
    )


def halves(value):
    high = value.astype(jnp.bfloat16)
    return high, (value - high.astype(jnp.float32)).astype(jnp.bfloat16)


def dot3(first, second, first_dim=1):
    if not isinstance(first, tuple):
        first = halves(first)
    if not isinstance(second, tuple):
        second = halves(second)

    def one(a, b):
        return lax.dot_general(
            a, b, (((first_dim,), (0,)), ((), ())), preferred_element_type=jnp.float32
        )

    return one(first[0], second[0]) + (one(first[0], second[1]) + one(first[1], second[0]))


def iota(shape, dim):
    return lax.broadcasted_iota(jnp.int32, shape, dim)


class Plan:
    def __init__(self, rows, cols, shape):
        self.rows, self.cols = rows, cols
        self.cycles, self.col_cycles, self.tile, _ = shape
        self.nx = 1
        while 2 * (2 * self.nx) ** 2 <= rows:
            self.nx *= 2
        self.nz = rows // self.nx
        self.owners = NB // self.tile
        self.owner_z = self.owners // self.nx
        self.panels = NB // LANES
        self.ny = cols // 2
        self.left = self.col_cycles * cols * LANES - 2 * NB


class ColumnGather:
    def __init__(self, plan, col, full, send, pair, forward, recv):
        self.plan, self.col, self.full = plan, col, full
        self.send, self.pair, self.forward, self.recv = send, pair, forward, recv
        self.first = plan.cols - plan.panels
        self.y, self.core = col // 2, col % 2
        self.mine = col - self.first

    def slot(self, block):
        return self.full.at[:, :, pl.ds(pl.multiple_of(block * LANES, LANES), LANES)]

    def copy(self, src, block, send, col):
        return pltpu.make_async_remote_copy(
            src_ref=src,
            dst_ref=self.slot(block),
            send_sem=send,
            recv_sem=self.recv.at[block],
            device_id={"col": col},
            device_id_type=MESH,
        )

    def other(self, step):
        return (self.y + step) % self.plan.ny

    def copies(self, src):
        out = [
            self.copy(src, self.mine, self.send.at[step], self.other(step) * 2 + self.core)
            for step in range(1, self.plan.ny)
        ]
        out.append(self.copy(src, self.mine, self.pair, self.y * 2 + 1 - self.core))
        return out

    def own(self, src):
        return pltpu.make_async_copy(src, self.slot(self.mine), self.recv.at[self.mine])

    def start(self, src):
        @pl.when(self.mine >= 0)
        def _():
            for copy in self.copies(src):
                copy.start()
            self.own(src).start()

    def relay(self):
        for step in range(1, self.plan.ny):
            block = self.other(step) * 2 + self.core - self.first

            @pl.when(block >= 0)
            def _():
                copy = self.copy(
                    self.slot(block), block, self.forward.at[step], self.y * 2 + 1 - self.core
                )
                copy.wait_recv()
                copy.start()

    def finish(self, src):
        @pl.when(self.mine >= 0)
        def _():
            self.own(src).wait()

        for step in range(self.plan.ny):
            block = self.other(step) * 2 + 1 - self.core - self.first

            @pl.when(block >= 0)
            def _():
                self.copy(self.slot(block), block, self.pair, self.y * 2 + 1 - self.core).wait_recv()

    def drain(self, src):
        @pl.when(self.mine >= 0)
        def _():
            for copy in self.copies(src):
                copy.wait_send()

        for step in range(1, self.plan.ny):
            block = self.other(step) * 2 + self.core - self.first

            @pl.when(block >= 0)
            def _():
                self.copy(
                    self.slot(block), block, self.forward.at[step], self.y * 2 + 1 - self.core
                ).wait_send()


def invert(full, inverse):
    row, col = iota((LANES, LANES), 0), iota((LANES, LANES), 1)
    count = NB // LANES
    blocks = []
    for k in range(count):
        part = full[k * LANES : (k + 1) * LANES, k * LANES : (k + 1) * LANES]
        blocks.append((part, jnp.where(row == col, 1.0 / jnp.where(row == col, part, 1.0), 0.0)))
    size = 1
    while size < LANES:
        mask = (
            (row // (2 * size) == col // (2 * size))
            & (row // size % 2 == 1)
            & (col // size % 2 == 0)
        )
        half = [dot(jnp.where(mask, part, 0.0), inv) for part, inv in blocks]
        blocks = [(part, inv - dot(inv, other)) for (part, inv), other in zip(blocks, half)]
        size *= 2
    inverse[...] = jnp.zeros_like(inverse)
    for k in range(count):
        inverse[k * LANES : (k + 1) * LANES, k * LANES : (k + 1) * LANES] = blocks[k][1]
    while size < NB:
        for base in range(0, NB, 2 * size):
            top, low = slice(base, base + size), slice(base + size, base + 2 * size)
            inner = dot(full[low, top], inverse[top, top])
            inverse[low, top] = -dot(inverse[low, low], inner)
        size *= 2


def kernel(
    plan, factor_in, adjoint_in, out, factor, adjoint, in_sems,
    panel, top, diag, inv, inv_t, corner, spread, yval, ysum, xrecv, zrecv, starts, start_full,
    a_send, a_pair, a_fwd, a_recv, b_send, b_pair, b_fwd, b_recv, d_send, d_pair, d_fwd, d_recv,
    s_send, s_pair, s_fwd, s_recv,
    t_z, t_x, t_fwd, t_recv, x_send, x_recv, z_send, z_recv, r_send, r_recv,
):
    p = plan
    row, col = lax.axis_index("row"), lax.axis_index("col")
    z, x = row // p.nx, row % p.nx
    last = p.col_cycles - 1
    tile, depth = p.tile, (p.cycles - 1) * p.tile
    width = p.col_cycles * LANES
    owner = row - (p.rows - p.owners)
    first_z = p.nz - p.owner_z
    is_panel = col >= p.cols - p.panels
    mine = col - (p.cols - p.panels)
    order = [last] + list(range(last))

    load_factor = pltpu.make_async_copy(factor_in, factor, in_sems.at[0])
    load_adjoint = pltpu.make_async_copy(adjoint_in, adjoint, in_sems.at[1])
    load_factor.start()
    load_adjoint.start()
    barrier = pltpu.get_barrier_semaphore()
    for step in range(1, p.rows):
        pl.semaphore_signal(
            barrier, inc=1, device_id={"row": (row + step) % p.rows}, device_id_type=MESH
        )
    for step in range(1, p.cols):
        pl.semaphore_signal(
            barrier, inc=1, device_id={"col": (col + step) % p.cols}, device_id_type=MESH
        )
    pl.semaphore_wait(barrier, p.rows + p.cols - 2)

    def to_row(src, dst, send, recv, target):
        return pltpu.make_async_remote_copy(
            src_ref=src, dst_ref=dst, send_sem=send, recv_sem=recv,
            device_id={"row": target}, device_id_type=MESH,
        )

    load_factor.wait()

    def top_slot(index, e):
        return top.at[index, :, e * LANES : (e + 1) * LANES]

    def top_copies(e):
        src = factor.at[0, e]
        dst, recv = top_slot(owner, e), t_recv.at[e, owner]
        made = [
            to_row(src, dst, t_z.at[e, k], recv, (z + k) % p.nz * p.nx + x) for k in range(1, p.nz)
        ]
        return made + [
            to_row(src, dst, t_x.at[e, k], recv, z * p.nx + (x + k) % p.nx) for k in range(1, p.nx)
        ]

    def top_own(e):
        return pltpu.make_async_copy(factor.at[0, e], top_slot(owner, e), t_recv.at[e, owner])

    @pl.when(owner >= 0)
    def _():
        for e in order:
            for copy in top_copies(e):
                copy.start()
            top_own(e).start()

    load_adjoint.wait()
    cut = (p.cycles - 1) * 3 // 4
    gather_a = ColumnGather(p, col, panel.at[:cut], a_send, a_pair, a_fwd, a_recv)
    gather_b = ColumnGather(p, col, panel.at[cut:], b_send, b_pair, b_fwd, b_recv)
    a_src, b_src = adjoint.at[1 : 1 + cut, last], adjoint.at[1 + cut :, last]
    gather_a.start(a_src)

    def top_forward(e, zi, action):
        index = zi * p.nx + x

        @pl.when(z != first_z + zi)
        def _():
            slot = top_slot(index, e)
            for k in range(1, p.nx):
                copy = to_row(
                    slot, slot, t_fwd.at[e, zi, k], t_recv.at[e, index],
                    z * p.nx + (x + k) % p.nx,
                )
                action(copy, k)

    def relay(copy, k):
        if k == 1:
            copy.wait_recv()
        copy.start()

    def top_relay(e):
        for zi in range(p.owner_z):
            top_forward(e, zi, relay)

    def top_finish(e):
        @pl.when(owner >= 0)
        def _():
            top_own(e).wait()

        for zi in range(p.owner_z):
            for k in range(1, p.nx):
                index = zi * p.nx + (x + k) % p.nx
                slot = top_slot(index, e)
                to_row(slot, slot, t_x.at[e, k], t_recv.at[e, index], row).wait_recv()

    top_relay(last)
    top_finish(last)
    gather_d = ColumnGather(p, col, diag, d_send, d_pair, d_fwd, d_recv)
    d_src = top.at[:, :, last * LANES : width]
    gather_d.start(d_src)
    gather_b.start(b_src)
    gather_a.relay()
    for e in range(last):
        top_relay(e)
    gather_a.finish(a_src)

    def corner_part(begin, end):
        rows_of = (end - begin) * tile
        columns = [
            factor[1 + begin : 1 + end, e].reshape(rows_of, LANES) for e in range(p.col_cycles)
        ]
        return dot3(panel[begin:end].reshape(rows_of, NB), jnp.concatenate(columns, 1), 0)

    corner[...] = corner_part(0, cut)
    gather_d.relay()
    gather_d.finish(d_src)
    full = diag.reshape(NB, NB)
    invert(full, inv)
    inv_t[...] = inv[...].T.reshape(inv_t.shape)
    gather_b.relay()
    gather_b.finish(b_src)
    corner[...] += corner_part(cut, p.cycles - 1)

    def x_copy(e, k):
        target = (x + k) % p.nx
        return to_row(
            yval.at[e, target], xrecv.at[e, x], x_send.at[e, k], x_recv.at[e, x],
            z * p.nx + target,
        )

    inv_tv = halves(inv_t[...].reshape(NB, NB))

    def put(e, value):
        value = value.reshape(p.owner_z, p.nx, tile, LANES)
        for k in range(p.nx):
            yval[e, k] = value[:, k]
        for k in range(1, p.nx):
            x_copy(e, k).start()

    put(last, dot3(inv_tv, corner[:, last * LANES : width]))
    rest = dot3(inv_tv, corner[:, : last * LANES])
    for e in range(last):
        put(e, rest[:, e * LANES : (e + 1) * LANES])

    def z_copy(e, zi):
        return to_row(
            ysum.at[e, zi], zrecv.at[e, z], z_send.at[e, zi], z_recv.at[e, z],
            (first_z + zi) * p.nx + x,
        )

    def x_sum(e):
        total = yval[e, x]
        for k in range(1, p.nx):
            source = (x + k) % p.nx
            to_row(
                xrecv.at[e, source], xrecv.at[e, source], x_send.at[e, k], x_recv.at[e, source], row
            ).wait_recv()
            total = total + xrecv[e, source]
        ysum[e] = total
        for zi in range(p.owner_z):
            @pl.when(z != first_z + zi)
            def _():
                z_copy(e, zi).start()

    x_sum(last)
    for e in range(last):
        top_finish(e)
    rights = top[...].reshape(NB, width)
    unit = (iota((NB, LANES), 0) == mine * LANES + iota((NB, LANES), 1)).astype(jnp.float32)
    rights = jnp.concatenate(
        [rights[:, : last * LANES], jnp.where(is_panel, unit, rights[:, last * LANES :])], 1
    )
    spread[...] = dot3(inv[...], rights)

    def trail(begin, end):
        change = dot3(panel[begin:end].reshape((end - begin) * tile, NB), spread[...])
        change = change.reshape(end - begin, tile, width)
        for e in range(p.col_cycles):
            part = change[:, :, e * LANES : (e + 1) * LANES]
            moved = adjoint[1 + begin : 1 + end, e] - part
            if e == last:
                moved = jnp.where(is_panel, part, moved)
            out[1 + begin : 1 + end, e] = moved

    middle = (p.cycles - 1) // 2
    trail(0, middle)
    trail(middle, p.cycles - 1)

    def z_sum(e):
        total = ysum[e, owner // p.nx]
        for k in range(1, p.nz):
            source = (z + k) % p.nz
            to_row(
                zrecv.at[e, source], zrecv.at[e, source], z_send.at[e, 0], z_recv.at[e, source], row
            ).wait_recv()
            total = total + zrecv[e, source]
        return total

    def start_copies():
        first = p.rows - p.owners
        return [
            to_row(
                starts.at[owner], starts.at[owner], r_send.at[k], r_recv.at[owner],
                first + (owner + k) % p.owners,
            )
            for k in range(1, p.owners)
        ]

    lower = iota((tile, LANES), 0) + owner * tile >= iota((tile, LANES), 1) + mine * LANES
    gather_s = ColumnGather(p, col, start_full, s_send, s_pair, s_fwd, s_recv)

    @pl.when((owner >= 0) & is_panel)
    def _():
        starts[owner] = jnp.where(lower, adjoint[0, last] - z_sum(last), 0.0)
        for copy in start_copies():
            copy.start()

    for e in range(last):
        x_sum(e)

    @pl.when(owner < 0)
    def _():
        for e in range(p.col_cycles):
            rows_at = iota((tile, LANES), 0) + row * tile
            cols_at = iota((tile, LANES), 1) + (e * p.cols + col) * LANES - p.left
            out[0, e] = jnp.where(cols_at > rows_at, 0.0, adjoint[0, e])

    @pl.when(owner >= 0)
    def _():
        @pl.when(is_panel)
        def _():
            for k in range(1, p.owners):
                source = (owner + k) % p.owners
                to_row(
                    starts.at[source], starts.at[source], r_send.at[k], r_recv.at[source], row
                ).wait_recv()

        gather_s.start(starts)
        gather_s.relay()
        gather_s.finish(starts)
        product = dot3(full[...], start_full[...].reshape(NB, NB), 0)
        row_at, col_at = iota((NB, NB), 0), iota((NB, NB), 1)
        both = (
            jnp.where(row_at >= col_at, product, 0.0) + jnp.where(row_at > col_at, product, 0.0).T
        )
        changes = dot3(dot3(inv_t[owner], both), spread[...])
        for e in range(last):
            out[0, e] = adjoint[0, e] - z_sum(e) - changes[:, e * LANES : (e + 1) * LANES]

        part = changes[:, last * LANES :]

        @pl.when(is_panel)
        def _():
            equal = iota((tile, LANES), 0) + owner * tile == iota((tile, LANES), 1) + mine * LANES
            out[0, last] = jnp.where(lower, jnp.where(equal, 0.5 * part, part), 0.0)

        @pl.when(jnp.logical_not(is_panel))
        def _():
            out[0, last] = adjoint[0, last] - z_sum(last) - part

        gather_s.drain(starts)

        @pl.when(is_panel)
        def _():
            for copy in start_copies():
                copy.wait_send()

    gather_a.drain(a_src)
    gather_b.drain(b_src)
    gather_d.drain(d_src)
    for e in order:
        @pl.when(owner >= 0)
        def _():
            for copy in top_copies(e):
                copy.wait_send()

        for zi in range(p.owner_z):
            top_forward(e, zi, lambda copy, k: copy.wait_send())

            @pl.when(z != first_z + zi)
            def _():
                z_copy(e, zi).wait_send()

        for k in range(1, p.nx):
            x_copy(e, k).wait_send()


def local(rows, cols, factor, adjoint):
    factor = jnp.transpose(factor, (0, 2, 1, 3))
    adjoint = jnp.transpose(adjoint, (0, 2, 1, 3))
    p = Plan(rows, cols, factor.shape)
    n, cc, tile = p.cycles - 1, p.col_cycles, p.tile
    dma = pltpu.SemaphoreType.DMA
    column = [dma((p.ny,)), dma, dma((p.ny,)), dma((p.panels,))]
    vmem = lambda *shape: pltpu.VMEM(shape, jnp.float32)
    result = pl.pallas_call(
        functools.partial(kernel, p),
        out_shape=jax.ShapeDtypeStruct(factor.shape, jnp.float32),
        in_specs=[pl.BlockSpec(memory_space=pltpu.HBM)] * 2,
        out_specs=pl.BlockSpec(memory_space=pltpu.VMEM),
        scratch_shapes=[
            pltpu.VMEM(factor.shape, jnp.float32),
            pltpu.VMEM(factor.shape, jnp.float32),
            dma((2,)),
            vmem(n, tile, NB),
            vmem(p.owners, tile, cc * LANES),
            vmem(p.owners, tile, NB),
            vmem(NB, NB),
            vmem(p.owners, tile, NB),
            vmem(NB, cc * LANES),
            vmem(NB, cc * LANES),
            vmem(cc, p.nx, p.owner_z, tile, LANES),
            vmem(cc, p.owner_z, tile, LANES),
            vmem(cc, p.nx, p.owner_z, tile, LANES),
            vmem(cc, p.nz, tile, LANES),
            vmem(p.owners, tile, LANES),
            vmem(p.owners, tile, NB),
            *column, *column, *column, *column,
            dma((cc, p.nz)), dma((cc, p.nx)), dma((cc, p.owner_z, p.nx)), dma((cc, p.owners)),
            dma((cc, p.nx)), dma((cc, p.nx)), dma((cc, p.owner_z)), dma((cc, p.nz)),
            dma((p.owners,)), dma((p.owners,)),
        ],
        compiler_params=pltpu.CompilerParams(
            collective_id=0, has_side_effects=True, vmem_limit_bytes=67043328
        ),
    )(factor, adjoint)
    return jnp.transpose(result, (0, 2, 1, 3))


def solution(mesh):
    spec = P(None, "row", None, "col")
    step = functools.partial(local, mesh.shape["row"], mesh.shape["col"])
    return jax.shard_map(
        step, mesh=mesh, in_specs=(spec, spec), out_specs=spec, check_vma=False
    )
```

```python
import functools

import jax
import jax.numpy as jnp
from jax import lax
from jax.experimental import pallas as pl
from jax.experimental.pallas import tpu as pltpu
from jax.sharding import PartitionSpec as P

NB = 512
LANES = 128
MESH = pl.DeviceIdType.MESH


def dot(first, second, first_dim=1):
    return lax.dot_general(
        first,
        second,
        (((first_dim,), (0,)), ((), ())),
        precision=lax.Precision.HIGHEST,
        preferred_element_type=jnp.float32,
    )


def halves(value):
    high = value.astype(jnp.bfloat16)
    return high, (value - high.astype(jnp.float32)).astype(jnp.bfloat16)


def dot3(first, second, first_dim=1):
    if not isinstance(first, tuple):
        first = halves(first)
    if not isinstance(second, tuple):
        second = halves(second)

    def one(a, b):
        return lax.dot_general(
            a, b, (((first_dim,), (0,)), ((), ())), preferred_element_type=jnp.float32
        )

    return one(first[0], second[0]) + (one(first[0], second[1]) + one(first[1], second[0]))


def iota(shape, dim):
    return lax.broadcasted_iota(jnp.int32, shape, dim)


class Plan:
    def __init__(self, rows, cols, shape):
        self.rows, self.cols = rows, cols
        self.cycles, self.col_cycles, self.tile, _ = shape
        self.nx = 1
        while 2 * (2 * self.nx) ** 2 <= rows:
            self.nx *= 2
        self.nz = rows // self.nx
        self.owners = NB // self.tile
        self.owner_z = self.owners // self.nx
        self.panels = NB // LANES
        self.ny = cols // 2
        self.left = self.col_cycles * cols * LANES - 2 * NB


class ColumnGather:
    def __init__(self, plan, col, full, send, pair, forward, recv):
        self.plan, self.col, self.full = plan, col, full
        self.send, self.pair, self.forward, self.recv = send, pair, forward, recv
        self.first = plan.cols - plan.panels
        self.y, self.core = col // 2, col % 2
        self.mine = col - self.first

    def slot(self, block):
        return self.full.at[:, :, pl.ds(pl.multiple_of(block * LANES, LANES), LANES)]

    def copy(self, src, block, send, col):
        return pltpu.make_async_remote_copy(
            src_ref=src,
            dst_ref=self.slot(block),
            send_sem=send,
            recv_sem=self.recv.at[block],
            device_id={"col": col},
            device_id_type=MESH,
        )

    def other(self, step):
        return (self.y + step) % self.plan.ny

    def copies(self, src):
        out = [
            self.copy(src, self.mine, self.send.at[step], self.other(step) * 2 + self.core)
            for step in range(1, self.plan.ny)
        ]
        out.append(self.copy(src, self.mine, self.pair, self.y * 2 + 1 - self.core))
        return out

    def own(self, src):
        return pltpu.make_async_copy(src, self.slot(self.mine), self.recv.at[self.mine])

    def start(self, src):
        @pl.when(self.mine >= 0)
        def _():
            for copy in self.copies(src):
                copy.start()
            self.own(src).start()

    def relay(self):
        for step in range(1, self.plan.ny):
            block = self.other(step) * 2 + self.core - self.first

            @pl.when(block >= 0)
            def _():
                copy = self.copy(
                    self.slot(block), block, self.forward.at[step], self.y * 2 + 1 - self.core
                )
                copy.wait_recv()
                copy.start()

    def finish(self, src):
        @pl.when(self.mine >= 0)
        def _():
            self.own(src).wait()

        for step in range(self.plan.ny):
            block = self.other(step) * 2 + 1 - self.core - self.first

            @pl.when(block >= 0)
            def _():
                self.copy(self.slot(block), block, self.pair, self.y * 2 + 1 - self.core).wait_recv()

    def drain(self, src):
        @pl.when(self.mine >= 0)
        def _():
            for copy in self.copies(src):
                copy.wait_send()

        for step in range(1, self.plan.ny):
            block = self.other(step) * 2 + self.core - self.first

            @pl.when(block >= 0)
            def _():
                self.copy(
                    self.slot(block), block, self.forward.at[step], self.y * 2 + 1 - self.core
                ).wait_send()


def invert(full, inverse):
    row, col = iota((LANES, LANES), 0), iota((LANES, LANES), 1)
    count = NB // LANES
    blocks = []
    for k in range(count):
        part = full[k * LANES : (k + 1) * LANES, k * LANES : (k + 1) * LANES]
        blocks.append((part, jnp.where(row == col, 1.0 / jnp.where(row == col, part, 1.0), 0.0)))
    size = 1
    while size < LANES:
        mask = (
            (row // (2 * size) == col // (2 * size))
            & (row // size % 2 == 1)
            & (col // size % 2 == 0)
        )
        half = [dot(jnp.where(mask, part, 0.0), inv) for part, inv in blocks]
        blocks = [(part, inv - dot(inv, other)) for (part, inv), other in zip(blocks, half)]
        size *= 2
    inverse[...] = jnp.zeros_like(inverse)
    for k in range(count):
        inverse[k * LANES : (k + 1) * LANES, k * LANES : (k + 1) * LANES] = blocks[k][1]
    while size < NB:
        for base in range(0, NB, 2 * size):
            top, low = slice(base, base + size), slice(base + size, base + 2 * size)
            inner = dot(full[low, top], inverse[top, top])
            inverse[low, top] = -dot(inverse[low, low], inner)
        size *= 2


def kernel(
    plan, factor_in, adjoint_in, out, factor, adjoint, in_sems,
    panel, top, diag, inv, inv_t, corner, spread, yval, ysum, xrecv, zrecv, starts, start_full,
    a_send, a_pair, a_fwd, a_recv, b_send, b_pair, b_fwd, b_recv, d_send, d_pair, d_fwd, d_recv,
    s_send, s_pair, s_fwd, s_recv,
    t_z, t_x, t_fwd, t_recv, x_send, x_recv, z_send, z_recv, r_send, r_recv,
    low, low_send, low_recv,
):
    p = plan
    row, col = lax.axis_index("row"), lax.axis_index("col")
    z, x = row // p.nx, row % p.nx
    last = p.col_cycles - 1
    tile, depth = p.tile, (p.cycles - 1) * p.tile
    width = p.col_cycles * LANES
    owner = row - (p.rows - p.owners)
    first_z = p.nz - p.owner_z
    is_panel = col >= p.cols - p.panels
    mine = col - (p.cols - p.panels)
    order = [last] + list(range(last))

    load_factor = pltpu.make_async_copy(factor_in, factor, in_sems.at[0])
    load_adjoint = pltpu.make_async_copy(adjoint_in, adjoint, in_sems.at[1])
    load_factor.start()
    load_adjoint.start()
    barrier = pltpu.get_barrier_semaphore()
    for step in range(1, p.rows):
        pl.semaphore_signal(
            barrier, inc=1, device_id={"row": (row + step) % p.rows}, device_id_type=MESH
        )
    for step in range(1, p.cols):
        pl.semaphore_signal(
            barrier, inc=1, device_id={"col": (col + step) % p.cols}, device_id_type=MESH
        )
    pl.semaphore_wait(barrier, p.rows + p.cols - 2)

    def to_row(src, dst, send, recv, target):
        return pltpu.make_async_remote_copy(
            src_ref=src, dst_ref=dst, send_sem=send, recv_sem=recv,
            device_id={"row": target}, device_id_type=MESH,
        )

    load_factor.wait()

    def top_slot(index, e):
        return top.at[index, :, e * LANES : (e + 1) * LANES]

    def top_copies(e):
        src = factor.at[0, e]
        dst, recv = top_slot(owner, e), t_recv.at[e, owner]
        made = [
            to_row(src, dst, t_z.at[e, k], recv, (z + k) % p.nz * p.nx + x) for k in range(1, p.nz)
        ]
        return made + [
            to_row(src, dst, t_x.at[e, k], recv, z * p.nx + (x + k) % p.nx) for k in range(1, p.nx)
        ]

    def top_own(e):
        return pltpu.make_async_copy(factor.at[0, e], top_slot(owner, e), t_recv.at[e, owner])

    @pl.when(owner >= 0)
    def _():
        for e in order:
            for copy in top_copies(e):
                copy.start()
            top_own(e).start()

    load_adjoint.wait()
    cut = (p.cycles - 1) * 3 // 4
    gather_a = ColumnGather(p, col, panel.at[:cut], a_send, a_pair, a_fwd, a_recv)
    gather_b = ColumnGather(p, col, panel.at[cut:], b_send, b_pair, b_fwd, b_recv)
    a_src, b_src = adjoint.at[1 : 1 + cut, last], adjoint.at[1 + cut :, last]
    gather_a.start(a_src)

    def top_forward(e, zi, action):
        index = zi * p.nx + x

        @pl.when(z != first_z + zi)
        def _():
            slot = top_slot(index, e)
            for k in range(1, p.nx):
                copy = to_row(
                    slot, slot, t_fwd.at[e, zi, k], t_recv.at[e, index],
                    z * p.nx + (x + k) % p.nx,
                )
                action(copy, k)

    def relay(copy, k):
        if k == 1:
            copy.wait_recv()
        copy.start()

    def top_relay(e):
        for zi in range(p.owner_z):
            top_forward(e, zi, relay)

    def top_finish(e):
        @pl.when(owner >= 0)
        def _():
            top_own(e).wait()

        for zi in range(p.owner_z):
            for k in range(1, p.nx):
                index = zi * p.nx + (x + k) % p.nx
                slot = top_slot(index, e)
                to_row(slot, slot, t_x.at[e, k], t_recv.at[e, index], row).wait_recv()

    top_relay(last)
    top_finish(last)
    gather_d = ColumnGather(p, col, diag, d_send, d_pair, d_fwd, d_recv)
    d_src = top.at[:, :, last * LANES : width]
    gather_d.start(d_src)
    gather_b.start(b_src)
    gather_a.relay()
    for e in range(last):
        top_relay(e)
    gather_a.finish(a_src)

    def corner_part(begin, end):
        rows_of = (end - begin) * tile
        columns = [
            factor[1 + begin : 1 + end, e].reshape(rows_of, LANES) for e in range(p.col_cycles)
        ]
        return dot3(panel[begin:end].reshape(rows_of, NB), jnp.concatenate(columns, 1), 0)

    corner[...] = corner_part(0, cut)
    gather_d.relay()
    gather_d.finish(d_src)
    full = diag.reshape(NB, NB)
    invert(full, inv)
    inv_t[...] = inv[...].T.reshape(inv_t.shape)
    gather_b.relay()
    gather_b.finish(b_src)
    corner[...] += corner_part(cut, p.cycles - 1)

    def x_copy(e, k):
        target = (x + k) % p.nx
        return to_row(
            yval.at[e, target], xrecv.at[e, x], x_send.at[e, k], x_recv.at[e, x],
            z * p.nx + target,
        )

    inv_tv = halves(inv_t[...].reshape(NB, NB))

    def put(e, value):
        value = value.reshape(p.owner_z, p.nx, tile, LANES)
        for k in range(p.nx):
            yval[e, k] = value[:, k]
        for k in range(1, p.nx):
            x_copy(e, k).start()

    put(last, dot3(inv_tv, corner[:, last * LANES : width]))
    rest = dot3(inv_tv, corner[:, : last * LANES])
    for e in range(last):
        put(e, rest[:, e * LANES : (e + 1) * LANES])

    def z_copy(e, zi):
        return to_row(
            ysum.at[e, zi], zrecv.at[e, z], z_send.at[e, zi], z_recv.at[e, z],
            (first_z + zi) * p.nx + x,
        )

    def x_sum(e):
        total = yval[e, x]
        for k in range(1, p.nx):
            source = (x + k) % p.nx
            to_row(
                xrecv.at[e, source], xrecv.at[e, source], x_send.at[e, k], x_recv.at[e, source], row
            ).wait_recv()
            total = total + xrecv[e, source]
        ysum[e] = total

        @pl.when((z == 0) | (z >= first_z))
        def _():
            pass_on(e)

    def low_copy(e):
        return to_row(
            ysum.at[e], low.at[e], low_send.at[e], low_recv.at[e], (z + 1) % p.nz * p.nx + x
        )

    def pass_on(e):
        @pl.when(z < first_z - 1)
        def _():
            low_copy(e).start()

        for zi in range(p.owner_z):
            @pl.when((z >= first_z - 1) & (z != first_z + zi))
            def _():
                z_copy(e, zi).start()

    def fold(e):
        @pl.when((z > 0) & (z < first_z))
        def _():
            low_copy(e).wait_recv()
            ysum[e] += low[e]
            pass_on(e)

    x_sum(last)
    for e in range(last):
        top_finish(e)
    rights = top[...].reshape(NB, width)
    unit = (iota((NB, LANES), 0) == mine * LANES + iota((NB, LANES), 1)).astype(jnp.float32)
    rights = jnp.concatenate(
        [rights[:, : last * LANES], jnp.where(is_panel, unit, rights[:, last * LANES :])], 1
    )
    spread[...] = dot3(inv[...], rights)

    def trail(begin, end):
        change = dot3(panel[begin:end].reshape((end - begin) * tile, NB), spread[...])
        change = change.reshape(end - begin, tile, width)
        for e in range(p.col_cycles):
            part = change[:, :, e * LANES : (e + 1) * LANES]
            moved = adjoint[1 + begin : 1 + end, e] - part
            if e == last:
                moved = jnp.where(is_panel, part, moved)
            out[1 + begin : 1 + end, e] = moved

    middle = (p.cycles - 1) // 2
    trail(0, middle)
    trail(middle, p.cycles - 1)
    fold(last)

    def z_sum(e):
        mine_z = owner // p.nx
        total = ysum[e, mine_z]
        sources = [first_z - 1] if first_z else []
        sources += [first_z + (mine_z + k) % p.owner_z for k in range(1, p.owner_z)]
        for source in sources:
            to_row(
                zrecv.at[e, source], zrecv.at[e, source], z_send.at[e, 0], z_recv.at[e, source], row
            ).wait_recv()
            total = total + zrecv[e, source]
        return total

    def start_copies():
        first = p.rows - p.owners
        return [
            to_row(
                starts.at[owner], starts.at[owner], r_send.at[k], r_recv.at[owner],
                first + (owner + k) % p.owners,
            )
            for k in range(1, p.owners)
        ]

    lower = iota((tile, LANES), 0) + owner * tile >= iota((tile, LANES), 1) + mine * LANES
    gathers = []
    for k in range(p.owners):
        index = (owner + k) % p.owners
        block = pl.ds(index, 1)
        gather = ColumnGather(
            p, col, start_full.at[block], s_send.at[k], s_pair.at[k], s_fwd.at[k], s_recv.at[index]
        )
        gathers.append((gather, starts.at[block]))

    @pl.when((owner >= 0) & is_panel)
    def _():
        starts[owner] = jnp.where(lower, adjoint[0, last] - z_sum(last), 0.0)
        for copy in start_copies():
            copy.start()
        gathers[0][0].start(gathers[0][1])

    for e in range(last):
        x_sum(e)
    for e in range(last):
        fold(e)

    @pl.when(owner < 0)
    def _():
        for e in range(p.col_cycles):
            rows_at = iota((tile, LANES), 0) + row * tile
            cols_at = iota((tile, LANES), 1) + (e * p.cols + col) * LANES - p.left
            out[0, e] = jnp.where(cols_at > rows_at, 0.0, adjoint[0, e])

    @pl.when(owner >= 0)
    def _():
        for k, (gather, src) in enumerate(gathers):
            if k:
                source = (owner + k) % p.owners

                @pl.when(is_panel)
                def _():
                    to_row(
                        starts.at[source], starts.at[source], r_send.at[k], r_recv.at[source], row
                    ).wait_recv()

                gather.start(src)
                gathers[k - 1][0].relay()
        gathers[-1][0].relay()
        for gather, src in gathers:
            gather.finish(src)
        product = dot3(full[...], start_full[...].reshape(NB, NB), 0)
        row_at, col_at = iota((NB, NB), 0), iota((NB, NB), 1)
        both = (
            jnp.where(row_at >= col_at, product, 0.0) + jnp.where(row_at > col_at, product, 0.0).T
        )
        changes = dot3(dot3(inv_t[owner], both), spread[...])
        for e in range(last):
            out[0, e] = adjoint[0, e] - z_sum(e) - changes[:, e * LANES : (e + 1) * LANES]

        part = changes[:, last * LANES :]

        @pl.when(is_panel)
        def _():
            equal = iota((tile, LANES), 0) + owner * tile == iota((tile, LANES), 1) + mine * LANES
            out[0, last] = jnp.where(lower, jnp.where(equal, 0.5 * part, part), 0.0)

        @pl.when(jnp.logical_not(is_panel))
        def _():
            out[0, last] = adjoint[0, last] - z_sum(last) - part

        for gather, src in gathers:
            gather.drain(src)

        @pl.when(is_panel)
        def _():
            for copy in start_copies():
                copy.wait_send()

    gather_a.drain(a_src)
    gather_b.drain(b_src)
    gather_d.drain(d_src)
    for e in order:
        @pl.when(owner >= 0)
        def _():
            for copy in top_copies(e):
                copy.wait_send()

        for zi in range(p.owner_z):
            top_forward(e, zi, lambda copy, k: copy.wait_send())

            @pl.when((z >= first_z - 1) & (z != first_z + zi))
            def _():
                z_copy(e, zi).wait_send()

        @pl.when(z < first_z - 1)
        def _():
            low_copy(e).wait_send()

        for k in range(1, p.nx):
            x_copy(e, k).wait_send()


def local(rows, cols, factor, adjoint):
    factor = jnp.transpose(factor, (0, 2, 1, 3))
    adjoint = jnp.transpose(adjoint, (0, 2, 1, 3))
    p = Plan(rows, cols, factor.shape)
    n, cc, tile = p.cycles - 1, p.col_cycles, p.tile
    dma = pltpu.SemaphoreType.DMA
    column = [dma((p.ny,)), dma, dma((p.ny,)), dma((p.panels,))]
    vmem = lambda *shape: pltpu.VMEM(shape, jnp.float32)
    result = pl.pallas_call(
        functools.partial(kernel, p),
        out_shape=jax.ShapeDtypeStruct(factor.shape, jnp.float32),
        in_specs=[pl.BlockSpec(memory_space=pltpu.HBM)] * 2,
        out_specs=pl.BlockSpec(memory_space=pltpu.VMEM),
        scratch_shapes=[
            pltpu.VMEM(factor.shape, jnp.float32),
            pltpu.VMEM(factor.shape, jnp.float32),
            dma((2,)),
            vmem(n, tile, NB),
            vmem(p.owners, tile, cc * LANES),
            vmem(p.owners, tile, NB),
            vmem(NB, NB),
            vmem(p.owners, tile, NB),
            vmem(NB, cc * LANES),
            vmem(NB, cc * LANES),
            vmem(cc, p.nx, p.owner_z, tile, LANES),
            vmem(cc, p.owner_z, tile, LANES),
            vmem(cc, p.nx, p.owner_z, tile, LANES),
            vmem(cc, p.nz, tile, LANES),
            vmem(p.owners, tile, LANES),
            vmem(p.owners, tile, NB),
            *column, *column, *column,
            dma((p.owners, p.ny)), dma((p.owners,)), dma((p.owners, p.ny)),
            dma((p.owners, p.panels)),
            dma((cc, p.nz)), dma((cc, p.nx)), dma((cc, p.owner_z, p.nx)), dma((cc, p.owners)),
            dma((cc, p.nx)), dma((cc, p.nx)), dma((cc, p.owner_z)), dma((cc, p.nz)),
            dma((p.owners,)), dma((p.owners,)),
            vmem(cc, p.owner_z, tile, LANES), dma((cc,)), dma((cc,)),
        ],
        compiler_params=pltpu.CompilerParams(
            collective_id=0, has_side_effects=True, vmem_limit_bytes=67043328
        ),
    )(factor, adjoint)
    return jnp.transpose(result, (0, 2, 1, 3))


def solution(mesh):
    spec = P(None, "row", None, "col")
    step = functools.partial(local, mesh.shape["row"], mesh.shape["col"])
    return jax.shard_map(
        step, mesh=mesh, in_specs=(spec, spec), out_specs=spec, check_vma=False
    )
```
